256 devices in a mesh: pb: 64 (over x, y, z_hi, core), ga: 4 (over z_lo).
Axes of the slice: x: 4, y: 4, z: 8 (z_hi: 2, z_lo: 4; z = z_hi * 4 + z_lo), core: 2. Of those that a mesh axis runs over, the one named last changes fastest.
Arguments:
- query_points: float32 [3, 262144], P(None, 'pb'), may hold values from 0 to 1
- cotangent: bfloat16 [64, 262144], P(None, 'pb'), may hold values from -6 to 6
- slab_ids: int32 [8, 262144], P(None, 'pb'), may hold values from -1 to 3
- rel_cells: int32 [8, 262144], P(None, 'pb'), may hold values from 0 to 511
- offsets: int32 [4, 2048], P('ga', 'pb'), may hold values from 0 to 15872
- latent: bfloat16 [4, 64, 16384], P('ga', None, 'pb'), may hold values from -6 to 6
- w_in: float32 [80, 6], replicated, may hold values from -2.5 to 2.5
- b_in: float32 [80], replicated, may hold values from -3 to 3
- w_out: bfloat16 [64, 80], replicated, may hold values from -0.625 to 0.625
- b_out: float32 [64], replicated, may hold values from -3 to 3
Outputs:
- grid_grad: float32 [4, 64, 16384], P('ga', None, 'pb')
- w_in_grad: float32 [80, 6], replicated
- b_in_grad: float32 [80], replicated
- w_out_grad: float32 [64, 80], replicated
- b_out_grad: float32 [64], replicated
The draws below stay inside these ranges and needn't reach their ends.
Inputs may be any that keep to these rules, and one draw needn't show every extreme that they name: `slab_ids`: -1 marks a padding slot; otherwise the slab that holds the neighbour cell.
All inputs are finite; a program needn't handle non-finite values.
Results may differ from the reference program's by a relative error of at most 0.0085.
Values may be sent and summed in bfloat16 or wider, within the bound.
A program may use at most 64 MiB of HBM per device.

```python
import math
import jax
import jax.numpy as jnp
from jax import lax

CH = 64
HID = 80
KN = 8
TILE = 128
WIN = 512
GX = 64
ZS = 4
SLAB_CELLS = 16384
QUERIES = 262144
TILES = 2048
N_GA = 4


def with_ends(array, rng, low, high):
    extent = array.shape
    spot = [jax.random.randint(jax.random.fold_in(rng, axis), (), 0, extent[axis]) for axis in range(len(extent))]
    array = array.at[tuple(spot)].set(low)
    longest = extent.index(max(extent))
    spot[longest] = (spot[longest] + 1) % extent[longest]
    return array.at[tuple(spot)].set(high)


def block_levels(rng, extent, split, least, top_value):
    loudness = 1.0
    for dim, blocks in split:
        draws = jax.random.uniform(jax.random.fold_in(jax.random.fold_in(rng, 6), dim), (blocks,), jnp.float32, least / len(split), top_value / len(split))
        loudness = loudness * jnp.repeat(jnp.exp(draws), extent[dim] // blocks).reshape((-1,) + (1,) * (len(extent) - 1 - dim))
    return loudness


def gaussian(rng, shape, deviation, bound, cuts=(), kind=jnp.bfloat16):
    drawn = jax.random.normal(rng, shape, jnp.float32) * deviation
    if len(cuts) > 0:
        drawn = block_levels(rng, shape, cuts, -0.22, 0.18) * drawn
    return jnp.clip(drawn, min=-bound, max=bound).astype(kind)


def setup_inputs(seed: int = 0) -> dict:
    key_list = jax.random.split(jax.random.key(seed), 11)
    return {
        "query_points": jnp.clip(1.0 * jax.random.uniform(key_list[0], (3, QUERIES), jnp.float32) ** block_levels(key_list[0], (3, QUERIES), ((1, 64),), -0.2, 0.2), 0.0, 1.0),
        "cotangent": gaussian(key_list[1], (CH, QUERIES), 1.0, 6.0, ((1, 64),)),
        "slab_ids": with_ends(jax.random.randint(key_list[2], (KN, QUERIES), -1, N_GA), jax.random.fold_in(key_list[2], 1), -1, N_GA - 1).astype(jnp.int32),
        "rel_cells": with_ends(jax.random.randint(key_list[3], (KN, QUERIES), 0, WIN), jax.random.fold_in(key_list[3], 1), 0, WIN - 1).astype(jnp.int32),
        "offsets": with_ends(jax.random.randint(key_list[4], (N_GA, TILES), 0, SLAB_CELLS - WIN + 1), jax.random.fold_in(key_list[4], 1), 0, SLAB_CELLS - WIN).astype(jnp.int32),
        "latent": gaussian(key_list[5], (N_GA, CH, SLAB_CELLS), 1.0, 6.0, ((0, 4), (2, 64))),
        "w_in": gaussian(key_list[6], (HID, 6), 6 ** -0.5, 2.5, (), jnp.float32),
        "b_in": gaussian(key_list[7], (HID,), 0.5, 3.0, (), jnp.float32),
        "w_out": gaussian(key_list[8], (CH, HID), HID ** -0.5, 0.625),
        "b_out": gaussian(key_list[9], (CH,), 0.5, 3.0, (), jnp.float32),
    }


def gelu_exact(values):
    return jax.nn.gelu(values, approximate=False)

def cell_centres(cell, slab):
    along_x = cell // (GX * ZS)
    along_y = cell // ZS % GX
    along_z = cell % ZS + slab * ZS
    return jnp.stack([(along_x.astype(jnp.float32) + 0.5) / GX, (along_y.astype(jnp.float32) + 0.5) / GX, (along_z.astype(jnp.float32) + 0.5) / GX], 0)

def reference(query_points, cotangent, slab_ids, rel_cells, offsets, latent, w_in, b_in, w_out, b_out):
    cells_slab = GX * GX * ZS
    latent_flat = jnp.transpose(latent, (1, 0, 2)).reshape(CH, N_GA * cells_slab)
    per_block = TILE * math.gcd(TILES, 64)
    count = QUERIES // per_block

    def reshape_blocks(values):
        return values.reshape(values.shape[0], count, per_block).transpose(1, 0, 2)

    def advance(running, inputs_block):
        grid_sum, totals = running
        number, points, cot_cols, slabs, rels = inputs_block
        tile_ids = (number * per_block + jnp.arange(per_block, dtype=jnp.int32)) // TILE
        slab_safe = jnp.maximum(slabs, 0)
        cell = offsets[slab_safe, tile_ids[None, :]] + rels
        flat_index = (slab_safe * cells_slab + cell).reshape(-1).astype(jnp.int32)
        mask_flat = (slabs >= 0).reshape(-1).astype(jnp.float32)
        centres = cell_centres(cell.reshape(-1), slab_safe.reshape(-1))
        features_in = jnp.concatenate([jnp.tile(points, (1, KN)), centres], 0)
        cot_flat = jnp.tile(cot_cols.astype(jnp.float32), (1, KN))
        feats = jnp.take(latent_flat, flat_index, axis=1).astype(jnp.float32)
        preact = jnp.dot(w_in, features_in, precision=lax.Precision.HIGHEST, preferred_element_type=jnp.float32) + b_in[:, None]
        hidden = gelu_exact(preact).astype(jnp.bfloat16)
        kernel = jnp.dot(w_out, hidden, preferred_element_type=jnp.float32) + b_out[:, None]
        grad_cell = (kernel * cot_flat * mask_flat).astype(jnp.bfloat16)
        grad_kernel = (feats * cot_flat * mask_flat).astype(jnp.bfloat16)
        grid_sum = grid_sum.at[:, flat_index].add(grad_cell.astype(jnp.float32))
        grad_w_out = lax.dot_general(grad_kernel, hidden, (((1,), (1,)), ((), ())), preferred_element_type=jnp.float32)
        grad_b_out = lax.optimization_barrier(jnp.sum(grad_kernel.astype(jnp.float32), 1))
        grad_hidden = lax.dot_general(w_out, grad_kernel, (((0,), (0,)), ((), ())), preferred_element_type=jnp.float32)
        grad_pre = jax.vjp(gelu_exact, preact)[1](grad_hidden)[0]
        grad_w_in = lax.dot_general(grad_pre, features_in, (((1,), (1,)), ((), ())), precision=lax.Precision.HIGHEST, preferred_element_type=jnp.float32)
        grad_b_in = lax.optimization_barrier(jnp.sum(grad_pre, 1))
        parts = (grad_w_in, grad_b_in, grad_w_out, grad_b_out)
        totals = tuple((old + new for old, new in zip(totals, parts)))
        return ((grid_sum, totals), None)
    start_totals = (jnp.zeros((HID, 6), jnp.float32), jnp.zeros((HID,), jnp.float32), jnp.zeros((CH, HID), jnp.float32), jnp.zeros((CH,), jnp.float32))
    start_grid = jnp.zeros((CH, N_GA * cells_slab), jnp.float32)
    inputs_all = (jnp.arange(count, dtype=jnp.int32), reshape_blocks(query_points), reshape_blocks(cotangent), reshape_blocks(slab_ids), reshape_blocks(rel_cells))
    (grid_sum, totals), _ = lax.scan(advance, (start_grid, start_totals), inputs_all)
    scale = float(QUERIES) ** (-0.5)
    grid_grad = grid_sum.reshape(CH, N_GA, cells_slab).transpose(1, 0, 2)
    return (grid_grad, totals[0] * scale, totals[1] * scale, totals[2] * scale, totals[3] * scale)
```

```python
import functools
import itertools
import math

import jax
import jax.numpy as jnp
from jax import lax
from jax.experimental import pallas as pl
from jax.experimental.pallas import tpu as pltpu
from jax.sharding import Mesh
from jax.sharding import PartitionSpec as P

KN = 8
TILE = 128
WIN = 512
GX = 64
ZS = 4
SPAN = WIN + TILE
BLOCK = 256
PB = ("pb_0", "pb_1", "pb_2", "pb_3")
PB_GA = ("pb_0", "pb_1", "pb_2", "pb_3", "ga")
F32 = jnp.float32
BF16 = jnp.bfloat16
I32 = jnp.int32
NT = (((1,), (1,)), ((), ()))
NN = (((1,), (0,)), ((), ()))


def dot(a, b, dims=NN):
    return lax.dot_general(a, b, dims, preferred_element_type=F32)


def split3(value):
    hi = value.astype(BF16)
    rest = value - hi.astype(F32)
    mid = rest.astype(BF16)
    low = (rest - mid.astype(F32)).astype(BF16)
    return hi, mid, low


def iota(shape, dim):
    return lax.broadcasted_iota(I32, shape, dim)


def unit(shape, row_to_col):
    return jnp.where(row_to_col(iota(shape, 0), iota(shape, 1)), 1.0, 0.0).astype(BF16)


def first_cell(start, cells):
    return jnp.minimum(start // TILE * TILE, cells - SPAN)


def weight_prologue(w_in_ref, b_in_ref, w_out_ref, b_out_ref, a_ref, wo_ref, wt_ref):
    hid = w_in_ref.shape[0]
    ch = w_out_ref.shape[0]
    parts = split3(w_in_ref[...])
    bias = split3(b_in_ref[...])
    total = jnp.zeros((hid, 48), F32)
    for n in range(3):
        place = unit(
            (6, 48),
            lambda r, c, n=n: (c // 16 == n)
            & (((r < 3) & (c % 16 < 9) & (c % 16 % 3 == r)) | ((r >= 3) & (c % 16 == r + 6))),
        )
        total += dot(parts[n], place)
        diag = jnp.where(
            iota((hid, hid), 0) == iota((hid, hid), 1), jnp.broadcast_to(bias[n].astype(F32), (hid, hid)), 0.0
        ).astype(BF16)
        total += dot(diag, unit((hid, 48), lambda r, c, n=n: c == 16 * n + 12))
    a_ref[...] = total.astype(BF16)
    bias = split3(b_out_ref[...])
    total = dot(w_out_ref[...], unit((hid, hid + 16), lambda r, c: r == c))
    for n in range(3):
        diag = jnp.where(
            iota((ch, ch), 0) == iota((ch, ch), 1), jnp.broadcast_to(bias[n].astype(F32), (ch, ch)), 0.0
        ).astype(BF16)
        total += dot(diag, unit((ch, hid + 16), lambda r, c, n=n: c == hid + n))
    wo_ref[...] = total.astype(BF16)
    wt_ref[...] = dot(unit((hid, hid), lambda r, c: r == c), w_out_ref[...], NT).astype(BF16)


def compact(slab_here, slab_ref, rel_ref, info_ref, count_ref):
    tiles = slab_ref.shape[1] // TILE
    group = 8
    rows = group * KN
    upper = unit((TILE, TILE), lambda r, c: r < c)
    ones = jnp.ones((TILE, TILE), BF16)
    earlier = unit((rows, rows), lambda r, c: (r // KN == c // KN) & (c < r))
    same = unit((rows, rows), lambda r, c: r // KN == c // KN)
    lane = iota((rows, TILE), 1)
    counts = []
    for g in range(tiles // group):
        cut = [slice((g * group + n) * TILE, (g * group + n + 1) * TILE) for n in range(group)]
        slabs = jnp.concatenate([slab_ref[:, c] for c in cut], 0)
        rels = jnp.concatenate([rel_ref[:, c] for c in cut], 0)
        live = slabs == slab_here
        live_b = jnp.where(live, 1.0, 0.0).astype(BF16)
        before = dot(live_b, upper).astype(I32)
        row_count = dot(live_b, ones)
        row_start = dot(earlier, row_count.astype(BF16)).astype(I32)
        counts.append(dot(same, row_count.astype(BF16)))
        row_count = row_count.astype(I32)
        item = jnp.where(live, (1 + rels + 1024 * lane) * 128 + (lane - before), 0)
        for bit in range(7):
            step = 1 << bit
            moved = pltpu.roll(item, TILE - step, 1)
            arrives = (moved & step) != 0
            leaves = (item & step) != 0
            item = jnp.where(arrives, moved, jnp.where(leaves, 0, item))
        value = item // 128
        for bit in range(7):
            step = 1 << bit
            value = jnp.where((row_start & step) != 0, pltpu.roll(value, step, 1), value)
        turn = row_start & (TILE - 1)
        number = (lane - turn) & (TILE - 1)
        place = number + row_start
        value = jnp.where(number < row_count, value, 0).astype(F32)
        chunk = place // TILE
        for n in range(group):
            part = slice(n * KN, (n + 1) * KN)
            dense = [
                jnp.sum(jnp.where(chunk[part] == c, value[part], 0.0), axis=0, keepdims=True)
                for c in range(KN)
            ]
            info_ref[g * group + n] = jnp.concatenate(dense, 0)
    for g in range(tiles // group):
        count_ref[g * rows : (g + 1) * rows] = counts[g].astype(I32)


def entry_rows(info, base, slab_here):
    packed = info.astype(I32) - 1
    valid = info > 0.0
    query = jnp.where(valid, packed >> 10, -1)
    rel = jnp.where(valid, packed & 1023, -1)
    cell = base + rel
    return query, rel, cell


def one_hot(index, rows):
    pieces = []
    for first in range(0, rows, TILE):
        near = index - first
        near = jnp.where((near >= 0) & (near < TILE), near, -1).astype(F32).astype(BF16)
        ids = iota((TILE, index.shape[1]), 0).astype(F32).astype(BF16)
        pieces.append(jnp.where(ids == jnp.broadcast_to(near, ids.shape), jnp.ones((), BF16), jnp.zeros((), BF16)))
    return jnp.concatenate(pieces, 0)


def block_forward(info, shift, base, slab_here, query_cols, a_ref, wo_ref):
    hid = a_ref.shape[0]
    query, rel, cell = entry_rows(info, base, slab_here)
    rel = jnp.where(rel >= 0, rel + shift, -1)
    cell = cell + shift
    ch = wo_ref.shape[0]
    here = dot(query_cols, one_hot(query, TILE))
    cot = here[:ch]
    point = here[ch : ch + 16]
    along_x = ((cell >> 8).astype(F32) + 0.5) / GX
    along_y = (((cell >> 2) & (GX - 1)).astype(F32) + 0.5) / GX
    along_z = ((cell & (ZS - 1)).astype(F32) + (slab_here * ZS).astype(F32) + 0.5) / GX
    row = iota((16, info.shape[1]), 0)
    features = jnp.where(
        row < 9,
        point,
        jnp.where(
            row == 9,
            along_x,
            jnp.where(row == 10, along_y, jnp.where(row == 11, along_z, jnp.where(row == 12, 1.0, 0.0))),
        ),
    ).astype(BF16)
    preact = dot(a_ref[...], jnp.concatenate([features] * 3, 0))
    cdf = 0.5 * (1.0 + lax.erf(preact * math.sqrt(0.5)))
    slope = cdf + preact * jnp.exp(preact * preact * -0.5) * (1.0 / math.sqrt(2.0 * math.pi))
    hidden = (preact * cdf).astype(BF16)
    extra = jnp.where(iota((16, info.shape[1]), 0) < 3, 1.0, 0.0).astype(BF16)
    hidden = jnp.concatenate([hidden, extra], 0)
    kernel = dot(wo_ref[...], hidden)
    grad_cell = (kernel * cot).astype(BF16)
    return rel, cot, features, slope, hidden, grad_cell


def compute_kernel(
    offsets_ref, points_ref, cot_ref, slab_ref, rel_ref, feats_ref,
    w_in_ref, b_in_ref, w_out_ref, b_out_ref,
    partial_ref, totals_ref,
    acc_ref, info_ref, count_ref, count_smem, a_ref, wo_ref, wt_ref, sem,
):
    slab_here = lax.axis_index("ga")
    cells = acc_ref.shape[1]
    ch = cot_ref.shape[0]
    hid = w_in_ref.shape[0]
    tiles = slab_ref.shape[1] // TILE
    weight_prologue(w_in_ref, b_in_ref, w_out_ref, b_out_ref, a_ref, wo_ref, wt_ref)
    compact(slab_here, slab_ref, rel_ref, info_ref, count_ref)
    copy = pltpu.make_async_copy(count_ref, count_smem, sem)
    copy.start()
    acc_ref[...] = jnp.zeros_like(acc_ref)
    totals_ref[...] = jnp.zeros_like(totals_ref)
    copy.wait()

    def tile_step(t, carry):
        lanes = pl.ds(pl.multiple_of(t * TILE, TILE), TILE)
        start = offsets_ref[0, t]
        base = pl.multiple_of(first_cell(start, cells), TILE)
        shift = start - base
        q_hi, q_mid, q_low = split3(points_ref[:, lanes])
        parts = jnp.concatenate(
            [q_hi.astype(F32), q_mid.astype(F32), q_low.astype(F32), jnp.zeros((7, TILE), F32)], 0
        ).astype(BF16)
        query_cols = jnp.concatenate([cot_ref[:, lanes], parts], 0)
        window = pl.ds(base, SPAN)
        blocks = (count_smem[t * KN, 0] + (BLOCK - 1)) // BLOCK

        def block_step(n, carry):
            info = jnp.concatenate(
                [info_ref[t, pl.ds(2 * n, 1), :], info_ref[t, pl.ds(2 * n + 1, 1), :]], 1
            )
            rel, cot, features, slope, hidden, grad_cell = block_forward(
                info, shift, base, slab_here, query_cols, a_ref, wo_ref
            )
            spread = one_hot(rel, SPAN)
            acc_ref[:, window] += dot(grad_cell, spread, NT)
            feats = dot(feats_ref[:, window], spread)
            grad_kernel = (feats * cot).astype(BF16)
            totals_ref[0:ch, 0 : hid + 16] += dot(grad_kernel, hidden, NT)
            grad_pre = dot(wt_ref[...], grad_kernel) * slope
            hi = grad_pre.astype(BF16)
            low = (grad_pre - hi.astype(F32)).astype(BF16)
            totals_ref[ch : ch + 16, 0:hid] += dot(features, hi, NT) + dot(features, low, NT)
            return carry

        return lax.fori_loop(0, blocks, block_step, carry)

    lax.fori_loop(0, tiles, tile_step, 0)
    wide = partial_ref.shape[-1]
    for p, (x, y, h, c) in enumerate(itertools.product(range(4), range(4), range(2), range(2))):
        first, second = ((x, y), (y, x))[c]
        partial_ref[c, first, second, h] = acc_ref[:, p * wide : (p + 1) * wide].astype(BF16)


def local_work(offsets, points, cot, slabs, rels, feats, w_in, b_in, w_out, b_out):
    ch, hid = w_out.shape
    cells = feats.shape[1]
    tiles = slabs.shape[1] // TILE
    vmem = pl.BlockSpec(memory_space=pltpu.VMEM)
    smem = pl.BlockSpec(memory_space=pltpu.SMEM)
    return pl.pallas_call(
        compute_kernel,
        out_shape=(
            jax.ShapeDtypeStruct((2, 4, 4, 2, ch, cells // 64), BF16),
            jax.ShapeDtypeStruct((ch + 16, TILE), F32),
        ),
        in_specs=[smem] + [vmem] * 9,
        out_specs=(vmem, vmem),
        scratch_shapes=[
            pltpu.VMEM((ch, cells), F32),
            pltpu.VMEM((tiles, KN, TILE), F32),
            pltpu.VMEM((tiles * KN, TILE), I32),
            pltpu.SMEM((tiles * KN, TILE), I32),
            pltpu.VMEM((hid, 48), BF16),
            pltpu.VMEM((ch, hid + 16), BF16),
            pltpu.VMEM((hid, ch), BF16),
            pltpu.SemaphoreType.DMA,
        ],
        compiler_params=pltpu.CompilerParams(vmem_limit_bytes=40 << 20),
        cost_estimate=pl.CostEstimate(flops=10**9, bytes_accessed=10**7, transcendentals=0),
        name="local_work",
    )(offsets, points, cot, slabs, rels, feats, w_in, b_in, w_out, b_out)


MESH_ID = pl.DeviceIdType.MESH


class Place:
    def __init__(self):
        self.x, self.y, self.h, self.c = (lax.axis_index(name) for name in PB)
        self.g = lax.axis_index("ga")
        self.first = self.x * (1 - self.c) + self.y * self.c
        self.second = self.y * (1 - self.c) + self.x * self.c

    def at(self, first=None, second=None, h=None, c=None, g=None):
        first = self.first if first is None else first
        second = self.second if second is None else second
        core = self.c
        return (
            first * (1 - core) + second * core,
            second * (1 - core) + first * core,
            self.h if h is None else h,
            core if c is None else c,
            self.g if g is None else g,
        )

    def sibling(self):
        return (self.x, self.y, self.h, 1 - self.c, self.g)


def greet(devices):
    barrier = pltpu.get_barrier_semaphore()
    for device in devices:
        pl.semaphore_signal(barrier, inc=1, device_id=device, device_id_type=MESH_ID)
    pl.semaphore_wait(barrier, len(devices))


def gather_kernel(block_ref, out_ref, send_sem, recv_sem):
    me = Place()
    wide = block_ref.shape[1]
    sends = []

    def number(first, second, h, c):
        x = first * (1 - me.c) + second * me.c
        y = second * (1 - me.c) + first * me.c
        return ((x * 4 + y) * 2 + h) * 2 + c

    def spot(p):
        return out_ref.at[:, pl.ds(pl.multiple_of(p * wide, wide), wide)]

    def send(source, p, device):
        copy = pltpu.make_async_remote_copy(
            src_ref=source,
            dst_ref=spot(p),
            send_sem=send_sem.at[len(sends)],
            recv_sem=recv_sem.at[p],
            device_id=device,
            device_id_type=MESH_ID,
        )
        copy.start()
        sends.append(copy)

    def arrived(p):
        pltpu.make_async_remote_copy(
            src_ref=spot(p),
            dst_ref=spot(p),
            send_sem=send_sem.at[0],
            recv_sem=recv_sem.at[p],
            device_id=me.sibling(),
            device_id_type=MESH_ID,
        ).wait_recv()

    steps = (1, 3, 2)
    near = [me.at(first=(me.first + n) % 4) for n in steps]
    far = [me.at(second=(me.second + n) % 4) for n in steps]
    across = me.at(h=1 - me.h)
    greet([me.sibling(), across] + near + far)
    mine = number(me.first, me.second, me.h, me.c)
    for device in [across] + near + far + [me.sibling()]:
        send(block_ref, mine, device)
    out_ref[:, pl.ds(pl.multiple_of(mine * wide, wide), wide)] = block_ref[...]

    def pass_on(p, devices):
        arrived(p)
        for device in devices + [me.sibling()]:
            send(spot(p), p, device)

    other = 1 - me.h
    for n in steps:
        pass_on(number((me.first + n) % 4, me.second, me.h, me.c), far)
    pass_on(number(me.first, me.second, other, me.c), near + far)
    for n in steps:
        for m in (0, 1, 3, 2):
            pass_on(number((me.first + m) % 4, (me.second + n) % 4, me.h, me.c), [])
    for n in steps:
        pass_on(number((me.first + n) % 4, me.second, other, me.c), far)
    for n in steps:
        for m in (0, 1, 3, 2):
            pass_on(number((me.first + m) % 4, (me.second + n) % 4, other, me.c), [])
    for x in range(4):
        for y in range(4):
            for h in range(2):
                arrived(((x * 4 + y) * 2 + h) * 2 + 1 - me.c)
    for copy in sends:
        copy.wait_send()


def gather_slab(block, owners):
    ch, wide = block.shape
    vmem = pl.BlockSpec(memory_space=pltpu.VMEM)
    return pl.pallas_call(
        gather_kernel,
        out_shape=jax.ShapeDtypeStruct((ch, wide * owners), BF16),
        in_specs=[vmem],
        out_specs=vmem,
        scratch_shapes=[pltpu.SemaphoreType.DMA((63,)), pltpu.SemaphoreType.DMA((64,))],
        compiler_params=pltpu.CompilerParams(
            collective_id=0, has_side_effects=True, vmem_limit_bytes=16 << 20
        ),
        name="gather_slab",
    )(block)


def reduce_kernel(
    partial_ref, totals_ref, out_ref, sums_ref,
    r0_ref, s0_ref, r1_ref, s1_ref, r2_ref, s2_ref, r3_ref,
    ta_ref, tf_ref, ts_ref, tz_ref, th_ref,
    sem0, sem1, sem2, sem3, tsem_a, tsem_f, tsem_s, tsem_z, tsem_h,
):
    me = Place()
    half = ta_ref.shape[0]
    sends = []

    def send(source, target, sems, device, recv_index, send_index):
        copy = pltpu.make_async_remote_copy(
            src_ref=source,
            dst_ref=target,
            send_sem=sems.at[(0,) + send_index],
            recv_sem=sems.at[(1,) + recv_index],
            device_id=device,
            device_id_type=MESH_ID,
        )
        copy.start()
        sends.append(copy)

    def arrived(target, sems, recv_index):
        pltpu.make_async_remote_copy(
            src_ref=target,
            dst_ref=target,
            send_sem=sems.at[(0,) + recv_index],
            recv_sem=sems.at[(1,) + recv_index],
            device_id=me.sibling(),
            device_id_type=MESH_ID,
        ).wait_recv()

    steps = (2, 1, 3)
    firsts = [(me.first + n) % 4 for n in steps]
    seconds = [(me.second + n) % 4 for n in steps]
    depth = me.h * 4 + me.g
    depths = [(depth + n) % 8 for n in range(1, 8)]
    line = [me.at(h=d // 4, g=d % 4) for d in depths]
    across = me.at(h=1 - me.h)
    greet(
        [me.sibling()]
        + [me.at(first=f) for f in firsts]
        + [me.at(second=s) for s in seconds]
        + line
    )

    own_half = pl.ds(pl.multiple_of(me.c * half, 8), half)
    other_half = pl.ds(pl.multiple_of((1 - me.c) * half, 8), half)
    send(totals_ref.at[other_half], ta_ref, tsem_a, me.sibling(), (0,), (0,))
    for n in steps + (0,):
        f = (me.second + n) % 4
        send(partial_ref.at[1 - me.c, f], r0_ref.at[f], sem0, me.sibling(), (f,), (f,))
    for n, f in zip(steps, firsts):
        arrived(r0_ref.at[f], sem0, (f,))
        s0_ref[n - 1] = (partial_ref[me.c, f].astype(F32) + r0_ref[f].astype(F32)).astype(BF16)
        for m in steps + (0,):
            s = (me.second + m) % 4
            send(s0_ref.at[n - 1, s], r1_ref.at[3 - n, s], sem1, me.at(first=f), (3 - n, s), (n - 1, s))

    arrived(ta_ref, tsem_a, (0,))
    tf_ref[me.first] = totals_ref[own_half] + ta_ref[...]
    for n, f in zip(steps, firsts):
        send(tf_ref.at[me.first], tf_ref.at[me.first], tsem_f, me.at(first=f), (me.first,), (n,))

    arrived(r0_ref.at[me.first], sem0, (me.first,))

    def collect(s):
        total = partial_ref[me.c, me.first, s].astype(F32) + r0_ref[me.first, s].astype(F32)
        for n in range(3):
            arrived(r1_ref.at[n, s], sem1, (n, s))
            total += r1_ref[n, s].astype(F32)
        return total

    for n, s in zip(steps, seconds):
        s1_ref[n - 1] = collect(s).astype(BF16)
        send(s1_ref.at[n - 1], r2_ref.at[3 - n], sem2, me.at(second=s), (3 - n,), (n - 1,))
        if n == steps[0]:
            for f in firsts:
                arrived(tf_ref.at[f], tsem_f, (f,))
            ts_ref[me.second] = tf_ref[0] + tf_ref[1] + tf_ref[2] + tf_ref[3]
            for k, t in zip(steps, seconds):
                send(ts_ref.at[me.second], ts_ref.at[me.second], tsem_s, me.at(second=t), (me.second,), (k,))
    total = collect(me.second)
    for s in seconds:
        arrived(ts_ref.at[s], tsem_s, (s,))
    tz_ref[depth] = ts_ref[0] + ts_ref[1] + ts_ref[2] + ts_ref[3]
    for n, device in enumerate(line):
        send(tz_ref.at[depth], tz_ref.at[depth], tsem_z, device, (depth,), (n,))
    for n in range(3):
        arrived(r2_ref.at[n], sem2, (n,))
        total += r2_ref[n].astype(F32)
    s2_ref[...] = total
    s1_ref[3, 0] = s2_ref[1 - me.h].astype(BF16)
    send(s1_ref.at[3, 0], r3_ref, sem3, across, (0,), (0,))
    for d in depths:
        arrived(tz_ref.at[d], tsem_z, (d,))
    total = tz_ref[0]
    for d in range(1, 8):
        total += tz_ref[d]
    th_ref[me.c] = total
    send(th_ref.at[me.c], th_ref.at[me.c], tsem_h, me.sibling(), (me.c,), (0,))
    arrived(r3_ref, sem3, (0,))
    out_ref[...] = s2_ref[me.h] + r3_ref[...].astype(F32)
    arrived(th_ref.at[1 - me.c], tsem_h, (1 - me.c,))
    sums_ref[0:half] = th_ref[0]
    sums_ref[half : 2 * half] = th_ref[1]
    for copy in sends:
        copy.wait_send()


def reduce_all(partial, totals):
    ch, wide = partial.shape[-2:]
    rows, lanes = totals.shape
    half = rows // 2
    vmem = pl.BlockSpec(memory_space=pltpu.VMEM)
    dma = pltpu.SemaphoreType.DMA
    return pl.pallas_call(
        reduce_kernel,
        out_shape=(
            jax.ShapeDtypeStruct((ch, wide), F32),
            jax.ShapeDtypeStruct((rows, lanes), F32),
        ),
        in_specs=[vmem, vmem],
        out_specs=(vmem, vmem),
        scratch_shapes=[
            pltpu.VMEM((4, 4, 2, ch, wide), BF16),
            pltpu.VMEM((3, 4, 2, ch, wide), BF16),
            pltpu.VMEM((3, 4, 2, ch, wide), BF16),
            pltpu.VMEM((4, 2, ch, wide), BF16),
            pltpu.VMEM((3, 2, ch, wide), BF16),
            pltpu.VMEM((2, ch, wide), F32),
            pltpu.VMEM((ch, wide), BF16),
            pltpu.VMEM((half, lanes), F32),
            pltpu.VMEM((4, half, lanes), F32),
            pltpu.VMEM((4, half, lanes), F32),
            pltpu.VMEM((8, half, lanes), F32),
            pltpu.VMEM((2, half, lanes), F32),
            dma((2, 4)),
            dma((2, 3, 4)),
            dma((2, 3)),
            dma((2, 1)),
            dma((2, 1)),
            dma((2, 4)),
            dma((2, 4)),
            dma((2, 8)),
            dma((2, 2)),
        ],
        compiler_params=pltpu.CompilerParams(
            collective_id=1, has_side_effects=True, vmem_limit_bytes=24 << 20
        ),
        name="reduce_all",
    )(partial, totals)


def shards(query_points, cotangent, slab_ids, rel_cells, offsets, latent, w_in, b_in, w_out, b_out):
    ch, hid = w_out.shape
    slab_feats = gather_slab(latent[0], lax.axis_size(PB))
    partial, totals = local_work(
        offsets, query_points, cotangent, slab_ids, rel_cells, slab_feats, w_in, b_in[None], w_out, b_out[None]
    )
    owned, totals = reduce_all(partial, totals)
    scale = float(query_points.shape[1] * lax.axis_size(PB)) ** (-0.5)
    totals = totals * scale
    w_out_grad = totals[:ch, :hid]
    b_out_grad = totals[:ch, hid]
    rows = totals[ch:, :hid]
    w_in_grad = jnp.concatenate([rows[0:3] + rows[3:6] + rows[6:9], rows[9:12]], 0).T
    b_in_grad = rows[12]
    return owned[None], w_in_grad, b_in_grad, w_out_grad, b_out_grad


def solution(mesh):
    finer = Mesh(
        mesh.devices.reshape(4, 4, 2, 2, mesh.shape["ga"]), ("pb_0", "pb_1", "pb_2", "pb_3", "ga")
    )
    in_specs = (
        P(None, PB),
        P(None, PB),
        P(None, PB),
        P(None, PB),
        P("ga", PB),
        P("ga", None, PB),
        P(),
        P(),
        P(),
        P(),
    )
    out_specs = (P("ga", None, PB), P(), P(), P(), P())
    return jax.shard_map(
        shards, mesh=finer, in_specs=in_specs, out_specs=out_specs, check_vma=False
    )
```

```python
import functools
import itertools
import math

import jax
import jax.numpy as jnp
from jax import lax
from jax.experimental import pallas as pl
from jax.experimental.pallas import tpu as pltpu
from jax.sharding import Mesh
from jax.sharding import PartitionSpec as P

KN = 8
TILE = 128
WIN = 512
GX = 64
ZS = 4
SPAN = WIN + TILE
BLOCK = 256
GROUP = 4
PB = ("pb_0", "pb_1", "pb_2", "pb_3")
PB_GA = ("pb_0", "pb_1", "pb_2", "pb_3", "ga")
F32 = jnp.float32
BF16 = jnp.bfloat16
I32 = jnp.int32
NT = (((1,), (1,)), ((), ()))
NN = (((1,), (0,)), ((), ()))


def dot(a, b, dims=NN):
    return lax.dot_general(a, b, dims, preferred_element_type=F32)


def split3(value):
    hi = value.astype(BF16)
    rest = value - hi.astype(F32)
    mid = rest.astype(BF16)
    low = (rest - mid.astype(F32)).astype(BF16)
    return hi, mid, low


def iota(shape, dim):
    return lax.broadcasted_iota(I32, shape, dim)


def unit(shape, row_to_col):
    return jnp.where(row_to_col(iota(shape, 0), iota(shape, 1)), 1.0, 0.0).astype(BF16)


def first_cell(start, cells):
    return jnp.minimum(start // TILE * TILE, cells - SPAN)


def weight_prologue(w_in_ref, b_in_ref, w_out_ref, b_out_ref, a_ref, wo_ref, wt_ref):
    hid = w_in_ref.shape[0]
    ch = w_out_ref.shape[0]
    parts = split3(w_in_ref[...])
    bias = split3(b_in_ref[...])
    total = jnp.zeros((hid, 48), F32)
    for n in range(3):
        place = unit(
            (6, 48),
            lambda r, c, n=n: (c // 16 == n)
            & (((r < 3) & (c % 16 < 9) & (c % 16 % 3 == r)) | ((r >= 3) & (c % 16 == r + 6))),
        )
        total += dot(parts[n], place)
        diag = jnp.where(
            iota((hid, hid), 0) == iota((hid, hid), 1), jnp.broadcast_to(bias[n].astype(F32), (hid, hid)), 0.0
        ).astype(BF16)
        total += dot(diag, unit((hid, 48), lambda r, c, n=n: c == 16 * n + 12))
    a_ref[...] = total.astype(BF16)
    bias = split3(b_out_ref[...])
    total = dot(w_out_ref[...], unit((hid, hid + 16), lambda r, c: r == c))
    for n in range(3):
        diag = jnp.where(
            iota((ch, ch), 0) == iota((ch, ch), 1), jnp.broadcast_to(bias[n].astype(F32), (ch, ch)), 0.0
        ).astype(BF16)
        total += dot(diag, unit((ch, hid + 16), lambda r, c, n=n: c == hid + n))
    wo_ref[...] = total.astype(BF16)
    wt_ref[...] = dot(unit((hid, hid), lambda r, c: r == c), w_out_ref[...], NT).astype(BF16)


def compact(slab_here, slab_ref, rel_ref, info_ref, count_ref):
    tiles = slab_ref.shape[1] // TILE
    rows = tiles * KN
    upper = unit((TILE, TILE), lambda r, c: r < c)
    ones = jnp.ones((TILE, TILE), BF16)
    earlier = unit((rows, rows), lambda r, c: (r // KN == c // KN) & (c < r))
    lane = iota((rows, TILE), 1)
    cut = [slice(n * TILE, (n + 1) * TILE) for n in range(tiles)]
    live = jnp.concatenate([slab_ref[:, c] for c in cut], 0) == slab_here
    rels = jnp.concatenate([rel_ref[:, c] for c in cut], 0)
    live_b = jnp.where(live, 1.0, 0.0).astype(BF16)
    before = dot(live_b, upper).astype(I32)
    row_count = dot(live_b, ones)
    row_start = dot(earlier, row_count.astype(BF16)).astype(I32)
    count = dot(unit((tiles, rows), lambda r, c: c // KN == r), row_count.astype(BF16))
    count = jnp.where(iota((tiles, TILE), 0) == iota((tiles, TILE), 1), count, 0.0)
    count_ref[...] = jnp.broadcast_to(jnp.sum(count, axis=0, keepdims=True), (8, TILE)).astype(I32)
    row_count = row_count.astype(I32)
    item = jnp.where(live, (1 + rels + 1024 * lane) * 128 + (lane - before), 0)
    for bit in range(7):
        step = 1 << bit
        moved = pltpu.roll(item, TILE - step, 1)
        item = jnp.where((moved & step) != 0, moved, jnp.where((item & step) != 0, 0, item))
    value = item >> 7
    for bit in range(7):
        step = 1 << bit
        value = jnp.where((row_start & step) != 0, pltpu.roll(value, step, 1), value)
    number = (lane - row_start) & (TILE - 1)
    chunk = (number + row_start) >> 7
    value = jnp.where(number < row_count, value, 0).astype(F32)
    for n in range(tiles):
        part = slice(n * KN, (n + 1) * KN)
        dense = [
            jnp.sum(jnp.where(chunk[part] == c, value[part], 0.0), axis=0, keepdims=True)
            for c in range(KN)
        ]
        info_ref[n] = jnp.concatenate(dense, 0)


def one_hot(index, rows):
    ids = iota((TILE, index.shape[1]), 0).astype(F32).astype(BF16)
    pieces = []
    for first in range(0, rows, TILE):
        near = index - first
        near = jnp.where((near >= 0.0) & (near < TILE), near, -1.0).astype(BF16)
        pieces.append(jnp.where(ids == jnp.broadcast_to(near, ids.shape), jnp.ones((), BF16), jnp.zeros((), BF16)))
    return jnp.concatenate(pieces, 0)


def query_columns(points, cot):
    q_hi, q_mid, q_low = split3(points)
    parts = jnp.concatenate(
        [q_hi.astype(F32), q_mid.astype(F32), q_low.astype(F32), jnp.zeros((7, points.shape[1]), F32)], 0
    ).astype(BF16)
    return jnp.concatenate([cot, parts], 0)


def entries_forward(infos, starts, cells, slab_here, columns, a_ref, wo_ref):
    ch = wo_ref.shape[0]
    rels, centres, heres = [], [], []
    for info, start, column in zip(infos, starts, columns):
        packed = info.astype(I32) - 1
        valid = info > 0.0
        query = jnp.where(valid, packed >> 10, -1).astype(F32)
        own = packed & 1023
        cell = jnp.where(valid, start + own, 0)
        rels.append(jnp.where(valid, own + (start - first_cell(start, cells)), -1).astype(F32))
        centres.append(
            (
                ((cell >> 8).astype(F32) + 0.5) / GX,
                (((cell >> 2) & (GX - 1)).astype(F32) + 0.5) / GX,
                ((cell & (ZS - 1)).astype(F32) + (slab_here * ZS).astype(F32) + 0.5) / GX,
            )
        )
        heres.append(dot(column, one_hot(query, TILE)))
    features, preacts = [], []
    for here, (along_x, along_y, along_z) in zip(heres, centres):
        row = iota((16, here.shape[1]), 0)
        feature = jnp.where(
            row < 9,
            here[ch : ch + 16],
            jnp.where(
                row == 9,
                along_x,
                jnp.where(row == 10, along_y, jnp.where(row == 11, along_z, jnp.where(row == 12, 1.0, 0.0))),
            ),
        ).astype(BF16)
        features.append(feature)
        preacts.append(dot(a_ref[...], jnp.concatenate([feature] * 3, 0)))
    slopes, hiddens, kernels = [], [], []
    for preact in preacts:
        cdf = 0.5 + 0.5 * lax.erf(preact * math.sqrt(0.5))
        slopes.append(cdf + preact * (jnp.exp(preact * preact * -0.5) * (1.0 / math.sqrt(2.0 * math.pi))))
        extra = jnp.where(iota((16, preact.shape[1]), 0) < 3, 1.0, 0.0).astype(BF16)
        hiddens.append(jnp.concatenate([(preact * cdf).astype(BF16), extra], 0))
        kernels.append(dot(wo_ref[...], hiddens[-1]))
    cots = [here[:ch] for here in heres]
    grads = [(kernel * cot).astype(BF16) for kernel, cot in zip(kernels, cots)]
    return rels, cots, features, slopes, hiddens, grads


def entries_backward(windows, rels, cots, features, slopes, hiddens, wt_ref, totals_ref):
    ch = cots[0].shape[0]
    hid = slopes[0].shape[0]
    feats = [dot(window, one_hot(rel, SPAN)) for window, rel in zip(windows, rels)]
    grad_kernels = [(feat * cot).astype(BF16) for feat, cot in zip(feats, cots)]
    grad_pres = [dot(wt_ref[...], g) * slope for g, slope in zip(grad_kernels, slopes)]
    totals_ref[0:ch, 0 : hid + 16] += sum(dot(g, hidden, NT) for g, hidden in zip(grad_kernels, hiddens))
    small = None
    for feature, grad_pre in zip(features, grad_pres):
        hi = grad_pre.astype(BF16)
        low = (grad_pre - hi.astype(F32)).astype(BF16)
        term = dot(feature, hi, NT) + dot(feature, low, NT)
        small = term if small is None else small + term
    totals_ref[ch : ch + 16, 0:hid] += small


MESH_ID = pl.DeviceIdType.MESH


class Place:
    def __init__(self):
        self.x, self.y, self.h, self.c = (lax.axis_index(name) for name in PB)
        self.g = lax.axis_index("ga")
        self.first = self.x * (1 - self.c) + self.y * self.c
        self.second = self.y * (1 - self.c) + self.x * self.c

    def at(self, first=None, second=None, h=None, c=None, g=None):
        first = self.first if first is None else first
        second = self.second if second is None else second
        core = self.c
        return (
            first * (1 - core) + second * core,
            second * (1 - core) + first * core,
            self.h if h is None else h,
            core if c is None else c,
            self.g if g is None else g,
        )

    def sibling(self):
        return (self.x, self.y, self.h, 1 - self.c, self.g)


def greet(devices):
    barrier = pltpu.get_barrier_semaphore()
    for device in devices:
        pl.semaphore_signal(barrier, inc=1, device_id=device, device_id_type=MESH_ID)
    pl.semaphore_wait(barrier, len(devices))


def gather_kernel(
    offsets_ref, points_ref, cot_ref, slab_ref, rel_ref, w_in_ref, b_in_ref, w_out_ref, b_out_ref, block_ref,
    out_ref, spread_ref, info_ref, count_ref, near_ref, cots_ref, feature_ref, slope_ref, hidden_ref,
    a_ref, wo_ref, wt_ref,
    send_sem, recv_sem,
):
    me = Place()
    wide = block_ref.shape[1]
    cells = out_ref.shape[1]
    tiles = slab_ref.shape[1] // TILE
    sends = []

    def number(first, second, h, c):
        x = first * (1 - me.c) + second * me.c
        y = second * (1 - me.c) + first * me.c
        return ((x * 4 + y) * 2 + h) * 2 + c

    def spot(p):
        return out_ref.at[:, pl.ds(pl.multiple_of(p * wide, wide), wide)]

    def send(source, p, device):
        copy = pltpu.make_async_remote_copy(
            src_ref=source,
            dst_ref=spot(p),
            send_sem=send_sem.at[len(sends)],
            recv_sem=recv_sem.at[p],
            device_id=device,
            device_id_type=MESH_ID,
        )
        copy.start()
        sends.append(copy)

    def arrived(p):
        pltpu.make_async_remote_copy(
            src_ref=spot(p),
            dst_ref=spot(p),
            send_sem=send_sem.at[0],
            recv_sem=recv_sem.at[p],
            device_id=me.sibling(),
            device_id_type=MESH_ID,
        ).wait_recv()

    def forward(first_group, last_group):
        def group_step(g, carry):
            ids = [g * GROUP + n for n in range(GROUP)]
            columns = []
            for t in ids:
                lanes = pl.ds(pl.multiple_of(t * TILE, TILE), TILE)
                columns.append(query_columns(points_ref[:, lanes], cot_ref[:, lanes]))
            infos = [jnp.concatenate([info_ref[t, 0:1, :], info_ref[t, 1:2, :]], 1) for t in ids]
            results = entries_forward(
                infos, [offsets_ref[0, t] for t in ids], cells, me.g, columns, a_ref, wo_ref
            )
            for t, rel, cot, feature, slope, hidden, grad in zip(ids, *results):
                spread_ref[t] = dot(grad, one_hot(rel, SPAN), NT)
                near_ref[t] = rel
                cots_ref[t] = cot.astype(BF16)
                feature_ref[t] = feature
                slope_ref[t] = slope
                hidden_ref[t] = hidden
            return carry

        lax.fori_loop(first_group, last_group, group_step, 0)

    steps = (1, 3, 2)
    near = [me.at(first=(me.first + n) % 4) for n in steps]
    far = [me.at(second=(me.second + n) % 4) for n in steps]
    across = me.at(h=1 - me.h)
    greet([me.sibling(), across] + near + far)
    mine = number(me.first, me.second, me.h, me.c)
    for device in [across] + near + far + [me.sibling()]:
        send(block_ref, mine, device)
    out_ref[:, pl.ds(pl.multiple_of(mine * wide, wide), wide)] = block_ref[...]

    def pass_on(p, devices):
        arrived(p)
        for device in devices + [me.sibling()]:
            send(spot(p), p, device)

    other = 1 - me.h
    groups = tiles // GROUP
    weight_prologue(w_in_ref, b_in_ref, w_out_ref, b_out_ref, a_ref, wo_ref, wt_ref)
    compact(me.g, slab_ref, rel_ref, info_ref, count_ref)
    for n in steps:
        pass_on(number((me.first + n) % 4, me.second, me.h, me.c), far)
    forward(0, groups // 4)
    pass_on(number(me.first, me.second, other, me.c), near + far)
    forward(groups // 4, groups // 2)
    for n in steps:
        for m in (0, 1, 3, 2):
            pass_on(number((me.first + m) % 4, (me.second + n) % 4, me.h, me.c), [])
    forward(groups // 2, groups * 3 // 4)
    for n in steps:
        pass_on(number((me.first + n) % 4, me.second, other, me.c), far)
    forward(groups * 3 // 4, groups)
    for n in steps:
        for m in (0, 1, 3, 2):
            pass_on(number((me.first + m) % 4, (me.second + n) % 4, other, me.c), [])
    for x in range(4):
        for y in range(4):
            for h in range(2):
                arrived(((x * 4 + y) * 2 + h) * 2 + 1 - me.c)
    for copy in sends:
        copy.wait_send()


def gather_and_forward(offsets, points, cot, slabs, rels, w_in, b_in, w_out, b_out, block, owners):
    ch, wide = block.shape
    hid = w_in.shape[0]
    tiles = slabs.shape[1] // TILE
    vmem = pl.BlockSpec(memory_space=pltpu.VMEM)
    smem = pl.BlockSpec(memory_space=pltpu.SMEM)
    shape = jax.ShapeDtypeStruct
    return pl.pallas_call(
        gather_kernel,
        out_shape=(
            shape((ch, wide * owners), BF16),
            shape((tiles, ch, SPAN), F32),
            shape((tiles, KN, TILE), F32),
            shape((8, TILE), I32),
            shape((tiles, 1, BLOCK), F32),
            shape((tiles, ch, BLOCK), BF16),
            shape((tiles, 16, BLOCK), BF16),
            shape((tiles, hid, BLOCK), F32),
            shape((tiles, hid + 16, BLOCK), BF16),
            shape((hid, 48), BF16),
            shape((ch, hid + 16), BF16),
            shape((hid, ch), BF16),
        ),
        in_specs=[smem] + [vmem] * 9,
        out_specs=(vmem,) * 12,
        scratch_shapes=[pltpu.SemaphoreType.DMA((63,)), pltpu.SemaphoreType.DMA((64,))],
        compiler_params=pltpu.CompilerParams(
            collective_id=0, has_side_effects=True, vmem_limit_bytes=40 << 20
        ),
        name="gather_and_forward",
    )(offsets, points, cot, slabs, rels, w_in, b_in, w_out, b_out, block)


def local_kernel(
    offsets_ref, counts_ref, points_ref, cot_ref, feats_ref, spread_ref, info_ref, a_ref, wo_ref, wt_ref,
    partial_ref, totals_ref, window_ref,
    acc_ref,
):
    slab_here = lax.axis_index("ga")
    cells = acc_ref.shape[1]
    tiles = spread_ref.shape[0]
    acc_ref[...] = jnp.zeros_like(acc_ref)
    totals_ref[...] = jnp.zeros_like(totals_ref)

    def tile_step(t, carry):
        start = offsets_ref[0, t]
        window = pl.ds(pl.multiple_of(first_cell(start, cells), TILE), SPAN)
        acc_ref[:, window] += spread_ref[t]
        window_ref[t] = feats_ref[:, window]

        def block_step(n, carry):
            lanes = pl.ds(pl.multiple_of(t * TILE, TILE), TILE)
            columns = query_columns(points_ref[:, lanes], cot_ref[:, lanes])
            info = jnp.concatenate(
                [info_ref[t, pl.ds(2 * n, 1), :], info_ref[t, pl.ds(2 * n + 1, 1), :]], 1
            )
            rels, cots, features, slopes, hiddens, grads = entries_forward(
                [info], [start], cells, slab_here, [columns], a_ref, wo_ref
            )
            acc_ref[:, window] += dot(grads[0], one_hot(rels[0], SPAN), NT)
            entries_backward(
                [feats_ref[:, window]], rels, cots, features, slopes, hiddens, wt_ref, totals_ref
            )
            return carry

        return lax.fori_loop(1, (counts_ref[0, t] + (BLOCK - 1)) // BLOCK, block_step, carry)

    lax.fori_loop(0, tiles, tile_step, 0)
    wide = partial_ref.shape[-1]
    for p, (x, y, h, c) in enumerate(itertools.product(range(4), range(4), range(2), range(2))):
        first, second = ((x, y), (y, x))[c]
        partial_ref[c, first, second, h] = acc_ref[:, p * wide : (p + 1) * wide].astype(BF16)


def local_sums(offsets, counts, points, cot, feats, spread, info, a, wo, wt):
    ch, cells = feats.shape
    vmem = pl.BlockSpec(memory_space=pltpu.VMEM)
    smem = pl.BlockSpec(memory_space=pltpu.SMEM)
    return pl.pallas_call(
        local_kernel,
        out_shape=(
            jax.ShapeDtypeStruct((2, 4, 4, 2, ch, cells // 64), BF16),
            jax.ShapeDtypeStruct((ch + 16, TILE), F32),
            jax.ShapeDtypeStruct((spread.shape[0], ch, SPAN), BF16),
        ),
        in_specs=[smem, smem] + [vmem] * 8,
        out_specs=(vmem, vmem, vmem),
        scratch_shapes=[pltpu.VMEM((ch, cells), F32)],
        compiler_params=pltpu.CompilerParams(vmem_limit_bytes=40 << 20),
        name="local_sums",
    )(offsets, counts, points, cot, feats, spread, info, a, wo, wt)


def reduce_kernel(
    partial_ref, beyond_ref, window_ref, near_ref, cots_ref, feature_ref, slope_ref, hidden_ref, wt_ref,
    out_ref, sums_ref,
    totals_ref,
    r0_ref, s0_ref, r1_ref, s1_ref, r2_ref, s2_ref, r3_ref,
    ta_ref, tf_ref, ts_ref, tz_ref, th_ref,
    sem0, sem1, sem2, sem3, tsem_a, tsem_f, tsem_s, tsem_z, tsem_h,
):
    me = Place()
    half = ta_ref.shape[0]
    sends = []

    def send(source, target, sems, device, recv_index, send_index):
        copy = pltpu.make_async_remote_copy(
            src_ref=source,
            dst_ref=target,
            send_sem=sems.at[(0,) + send_index],
            recv_sem=sems.at[(1,) + recv_index],
            device_id=device,
            device_id_type=MESH_ID,
        )
        copy.start()
        sends.append(copy)

    def arrived(target, sems, recv_index):
        pltpu.make_async_remote_copy(
            src_ref=target,
            dst_ref=target,
            send_sem=sems.at[(0,) + recv_index],
            recv_sem=sems.at[(1,) + recv_index],
            device_id=me.sibling(),
            device_id_type=MESH_ID,
        ).wait_recv()

    steps = (2, 1, 3)
    firsts = [(me.first + n) % 4 for n in steps]
    seconds = [(me.second + n) % 4 for n in steps]
    depth = me.h * 4 + me.g
    depths = [(depth + n) % 8 for n in range(1, 8)]
    line = [me.at(h=d // 4, g=d % 4) for d in depths]
    across = me.at(h=1 - me.h)
    greet(
        [me.sibling()]
        + [me.at(first=f) for f in firsts]
        + [me.at(second=s) for s in seconds]
        + line
    )

    tiles = near_ref.shape[0]

    def backward(first_group, last_group):
        def group_step(g, carry):
            ids = [g * GROUP + n for n in range(GROUP)]
            entries_backward(
                [window_ref[t] for t in ids],
                [near_ref[t] for t in ids],
                [cots_ref[t].astype(F32) for t in ids],
                [feature_ref[t] for t in ids],
                [slope_ref[t] for t in ids],
                [hidden_ref[t] for t in ids],
                wt_ref,
                totals_ref,
            )
            return carry

        lax.fori_loop(first_group, last_group, group_step, 0)

    own_half = pl.ds(pl.multiple_of(me.c * half, 8), half)
    other_half = pl.ds(pl.multiple_of((1 - me.c) * half, 8), half)
    for n in steps + (0,):
        f = (me.second + n) % 4
        send(partial_ref.at[1 - me.c, f], r0_ref.at[f], sem0, me.sibling(), (f,), (f,))
    totals_ref[...] = beyond_ref[...]
    for n, f in zip(steps, firsts):
        arrived(r0_ref.at[f], sem0, (f,))
        s0_ref[n - 1] = (partial_ref[me.c, f].astype(F32) + r0_ref[f].astype(F32)).astype(BF16)
        for m in steps + (0,):
            s = (me.second + m) % 4
            send(s0_ref.at[n - 1, s], r1_ref.at[3 - n, s], sem1, me.at(first=f), (3 - n, s), (n - 1, s))

    backward(0, tiles // GROUP)
    send(totals_ref.at[other_half], ta_ref, tsem_a, me.sibling(), (0,), (0,))
    arrived(ta_ref, tsem_a, (0,))
    tf_ref[me.first] = totals_ref[own_half] + ta_ref[...]
    for n, f in zip(steps, firsts):
        send(tf_ref.at[me.first], tf_ref.at[me.first], tsem_f, me.at(first=f), (me.first,), (n,))

    arrived(r0_ref.at[me.first], sem0, (me.first,))

    def collect(s):
        total = partial_ref[me.c, me.first, s].astype(F32) + r0_ref[me.first, s].astype(F32)
        for n in range(3):
            arrived(r1_ref.at[n, s], sem1, (n, s))
            total += r1_ref[n, s].astype(F32)
        return total

    for n, s in zip(steps, seconds):
        s1_ref[n - 1] = collect(s).astype(BF16)
        send(s1_ref.at[n - 1], r2_ref.at[3 - n], sem2, me.at(second=s), (3 - n,), (n - 1,))
        if n == steps[0]:
            for f in firsts:
                arrived(tf_ref.at[f], tsem_f, (f,))
            ts_ref[me.second] = tf_ref[0] + tf_ref[1] + tf_ref[2] + tf_ref[3]
            for k, t in zip(steps, seconds):
                send(ts_ref.at[me.second], ts_ref.at[me.second], tsem_s, me.at(second=t), (me.second,), (k,))
    total = collect(me.second)
    for s in seconds:
        arrived(ts_ref.at[s], tsem_s, (s,))
    tz_ref[depth] = ts_ref[0] + ts_ref[1] + ts_ref[2] + ts_ref[3]
    for n, device in enumerate(line):
        send(tz_ref.at[depth], tz_ref.at[depth], tsem_z, device, (depth,), (n,))
    for n in range(3):
        arrived(r2_ref.at[n], sem2, (n,))
        total += r2_ref[n].astype(F32)
    s2_ref[...] = total
    s1_ref[3, 0] = s2_ref[1 - me.h].astype(BF16)
    send(s1_ref.at[3, 0], r3_ref, sem3, across, (0,), (0,))
    for d in depths:
        arrived(tz_ref.at[d], tsem_z, (d,))
    total = tz_ref[0]
    for d in range(1, 8):
        total += tz_ref[d]
    th_ref[me.c] = total
    send(th_ref.at[me.c], th_ref.at[me.c], tsem_h, me.sibling(), (me.c,), (0,))
    arrived(r3_ref, sem3, (0,))
    out_ref[...] = s2_ref[me.h] + r3_ref[...].astype(F32)
    arrived(th_ref.at[1 - me.c], tsem_h, (1 - me.c,))
    sums_ref[0:half] = th_ref[0]
    sums_ref[half : 2 * half] = th_ref[1]
    for copy in sends:
        copy.wait_send()


def reduce_and_backward(partial, totals, windows, near, cots, feature, slope, hidden, wt):
    ch, wide = partial.shape[-2:]
    rows, lanes = totals.shape
    half = rows // 2
    vmem = pl.BlockSpec(memory_space=pltpu.VMEM)
    dma = pltpu.SemaphoreType.DMA
    return pl.pallas_call(
        reduce_kernel,
        out_shape=(
            jax.ShapeDtypeStruct((ch, wide), F32),
            jax.ShapeDtypeStruct((rows, lanes), F32),
        ),
        in_specs=[vmem] * 9,
        out_specs=(vmem, vmem),
        scratch_shapes=[
            pltpu.VMEM((rows, lanes), F32),
            pltpu.VMEM((4, 4, 2, ch, wide), BF16),
            pltpu.VMEM((3, 4, 2, ch, wide), BF16),
            pltpu.VMEM((3, 4, 2, ch, wide), BF16),
            pltpu.VMEM((4, 2, ch, wide), BF16),
            pltpu.VMEM((3, 2, ch, wide), BF16),
            pltpu.VMEM((2, ch, wide), F32),
            pltpu.VMEM((ch, wide), BF16),
            pltpu.VMEM((half, lanes), F32),
            pltpu.VMEM((4, half, lanes), F32),
            pltpu.VMEM((4, half, lanes), F32),
            pltpu.VMEM((8, half, lanes), F32),
            pltpu.VMEM((2, half, lanes), F32),
            dma((2, 4)),
            dma((2, 3, 4)),
            dma((2, 3)),
            dma((2, 1)),
            dma((2, 1)),
            dma((2, 4)),
            dma((2, 4)),
            dma((2, 8)),
            dma((2, 2)),
        ],
        compiler_params=pltpu.CompilerParams(
            collective_id=1, has_side_effects=True, vmem_limit_bytes=40 << 20
        ),
        name="reduce_and_backward",
    )(partial, totals, windows, near, cots, feature, slope, hidden, wt)


def shards(query_points, cotangent, slab_ids, rel_cells, offsets, latent, w_in, b_in, w_out, b_out):
    ch, hid = w_out.shape
    feats, spread, info, counts, near, cots, feature, slope, hidden, a, wo, wt = gather_and_forward(
        offsets, query_points, cotangent, slab_ids, rel_cells,
        w_in, b_in[None], w_out, b_out[None], latent[0], lax.axis_size(PB),
    )
    partial, totals, windows = local_sums(offsets, counts, query_points, cotangent, feats, spread, info, a, wo, wt)
    owned, totals = reduce_and_backward(
        partial, totals, windows, near, cots, feature, slope, hidden, wt
    )
    scale = float(query_points.shape[1] * lax.axis_size(PB)) ** (-0.5)
    totals = totals * scale
    w_out_grad = totals[:ch, :hid]
    b_out_grad = totals[:ch, hid]
    rows = totals[ch:, :hid]
    w_in_grad = jnp.concatenate([rows[0:3] + rows[3:6] + rows[6:9], rows[9:12]], 0).T
    b_in_grad = rows[12]
    return owned[None], w_in_grad, b_in_grad, w_out_grad, b_out_grad


def solution(mesh):
    finer = Mesh(
        mesh.devices.reshape(4, 4, 2, 2, mesh.shape["ga"]), ("pb_0", "pb_1", "pb_2", "pb_3", "ga")
    )
    in_specs = (
        P(None, PB),
        P(None, PB),
        P(None, PB),
        P(None, PB),
        P("ga", PB),
        P("ga", None, PB),
        P(),
        P(),
        P(),
        P(),
    )
    out_specs = (P("ga", None, PB), P(), P(), P(), P())
    return jax.shard_map(
        shards, mesh=finer, in_specs=in_specs, out_specs=out_specs, check_vma=False
    )
```

```python
import functools
import itertools
import math

import jax
import jax.numpy as jnp
from jax import lax
from jax.experimental import pallas as pl
from jax.experimental.pallas import tpu as pltpu
from jax.sharding import Mesh
from jax.sharding import PartitionSpec as P

KN = 8
TILE = 128
WIN = 512
GX = 64
ZS = 4
SPAN = WIN + TILE
BLOCK = 256
GROUP = 4
PB = ("pb_0", "pb_1", "pb_2", "pb_3")
PB_GA = ("pb_0", "pb_1", "pb_2", "pb_3", "ga")
F32 = jnp.float32
BF16 = jnp.bfloat16
I32 = jnp.int32
NT = (((1,), (1,)), ((), ()))
NN = (((1,), (0,)), ((), ()))


def dot(a, b, dims=NN):
    return lax.dot_general(a, b, dims, preferred_element_type=F32)


def split3(value):
    hi = value.astype(BF16)
    rest = value - hi.astype(F32)
    mid = rest.astype(BF16)
    low = (rest - mid.astype(F32)).astype(BF16)
    return hi, mid, low


def iota(shape, dim):
    return lax.broadcasted_iota(I32, shape, dim)


def unit(shape, row_to_col):
    return jnp.where(row_to_col(iota(shape, 0), iota(shape, 1)), 1.0, 0.0).astype(BF16)


def first_cell(start, cells):
    return jnp.minimum(start // TILE * TILE, cells - SPAN)


def weight_prologue(w_in_ref, b_in_ref, w_out_ref, b_out_ref, a_ref, wo_ref, wt_ref):
    hid = w_in_ref.shape[1]
    ch = w_out_ref.shape[0]
    total = jnp.zeros((48, hid), F32)
    row = iota((48, hid), 0)
    for n, (weight, bias) in enumerate(zip(split3(w_in_ref[...]), split3(b_in_ref[...]))):
        place = unit(
            (48, 6),
            lambda c, r, n=n: (c // 16 == n)
            & (((r < 3) & (c % 16 < 9) & (c % 16 % 3 == r)) | ((r >= 3) & (c % 16 == r + 6))),
        )
        total += dot(place, weight)
        total += jnp.where(row == 16 * n + 12, bias.astype(F32), 0.0)
    same = unit((hid, hid), lambda r, c: r == c)
    a_ref[...] = dot(same, total.astype(BF16), NT).astype(BF16)
    wt_ref[...] = dot(same, w_out_ref[...], NT).astype(BF16)
    total = dot(w_out_ref[...], unit((hid, hid + 16), lambda r, c: r == c))
    for n, bias in enumerate(split3(b_out_ref[...])):
        diag = jnp.where(
            iota((ch, ch), 0) == iota((ch, ch), 1), jnp.broadcast_to(bias.astype(F32), (ch, ch)), 0.0
        ).astype(BF16)
        total += dot(diag, unit((ch, hid + 16), lambda r, c, n=n: c == hid + n))
    wo_ref[...] = total.astype(BF16)


def compact(slab_here, slab_ref, rel_ref, info_ref, count_ref):
    tiles = slab_ref.shape[1] // TILE
    rows = tiles * KN
    upper = unit((TILE, TILE), lambda r, c: r < c)
    ones = jnp.ones((TILE, TILE), BF16)
    earlier = unit((rows, rows), lambda r, c: (r // KN == c // KN) & (c < r))
    lane = iota((rows, TILE), 1)
    cut = [slice(n * TILE, (n + 1) * TILE) for n in range(tiles)]
    live = jnp.concatenate([slab_ref[:, c] for c in cut], 0) == slab_here
    rels = jnp.concatenate([rel_ref[:, c] for c in cut], 0)
    live_b = jnp.where(live, 1.0, 0.0).astype(BF16)
    before = dot(live_b, upper).astype(I32)
    row_count = dot(live_b, ones)
    row_start = dot(earlier, row_count.astype(BF16)).astype(I32)
    count = dot(unit((tiles, rows), lambda r, c: c // KN == r), row_count.astype(BF16))
    count = jnp.where(iota((tiles, TILE), 0) == iota((tiles, TILE), 1), count, 0.0)
    count_ref[...] = jnp.broadcast_to(jnp.sum(count, axis=0, keepdims=True), (8, TILE)).astype(I32)
    row_count = row_count.astype(I32)
    item = jnp.where(live, (1 + rels + 1024 * lane) * 128 + (lane - before), 0)
    for bit in range(7):
        step = 1 << bit
        moved = pltpu.roll(item, TILE - step, 1)
        item = jnp.where((moved & step) != 0, moved, jnp.where((item & step) != 0, 0, item))
    value = item >> 7
    for bit in range(7):
        step = 1 << bit
        value = jnp.where((row_start & step) != 0, pltpu.roll(value, step, 1), value)
    number = (lane - row_start) & (TILE - 1)
    chunk = (number + row_start) >> 7
    value = jnp.where(number < row_count, value, 0).astype(F32)
    for n in range(tiles):
        part = slice(n * KN, (n + 1) * KN)
        dense = [
            jnp.sum(jnp.where(chunk[part] == c, value[part], 0.0), axis=0, keepdims=True)
            for c in range(KN)
        ]
        info_ref[n] = jnp.concatenate(dense, 0)


def one_hot(index, rows):
    ids = iota((TILE, index.shape[1]), 0).astype(F32).astype(BF16)
    pieces = []
    for first in range(0, rows, TILE):
        near = index - first
        near = jnp.where((near >= 0.0) & (near < TILE), near, -1.0).astype(BF16)
        pieces.append(jnp.where(ids == jnp.broadcast_to(near, ids.shape), jnp.ones((), BF16), jnp.zeros((), BF16)))
    return jnp.concatenate(pieces, 0)


def query_columns(points, cot):
    q_hi, q_mid, q_low = split3(points)
    parts = jnp.concatenate(
        [q_hi.astype(F32), q_mid.astype(F32), q_low.astype(F32), jnp.zeros((7, points.shape[1]), F32)], 0
    ).astype(BF16)
    return jnp.concatenate([cot, parts], 0)


def entries_forward(infos, starts, cells, slab_here, columns, a_ref, wo_ref):
    ch = wo_ref.shape[0]
    rels, centres, heres = [], [], []
    for info, start, column in zip(infos, starts, columns):
        packed = info.astype(I32) - 1
        valid = info > 0.0
        query = jnp.where(valid, packed >> 10, -1).astype(F32)
        own = packed & 1023
        cell = jnp.where(valid, start + own, 0)
        rels.append(jnp.where(valid, own + (start - first_cell(start, cells)), -1).astype(F32))
        centres.append(
            (
                ((cell >> 8).astype(F32) + 0.5) / GX,
                (((cell >> 2) & (GX - 1)).astype(F32) + 0.5) / GX,
                ((cell & (ZS - 1)).astype(F32) + (slab_here * ZS).astype(F32) + 0.5) / GX,
            )
        )
        heres.append(dot(column, one_hot(query, TILE)))
    features, preacts = [], []
    for here, (along_x, along_y, along_z) in zip(heres, centres):
        row = iota((16, here.shape[1]), 0)
        feature = jnp.where(
            row < 9,
            here[ch : ch + 16],
            jnp.where(
                row == 9,
                along_x,
                jnp.where(row == 10, along_y, jnp.where(row == 11, along_z, jnp.where(row == 12, 1.0, 0.0))),
            ),
        ).astype(BF16)
        features.append(feature)
        preacts.append(dot(a_ref[...], jnp.concatenate([feature] * 3, 0)))
    slopes, hiddens, kernels = [], [], []
    for preact in preacts:
        cdf = 0.5 + 0.5 * lax.erf(preact * math.sqrt(0.5))
        slopes.append(cdf + preact * (jnp.exp(preact * preact * -0.5) * (1.0 / math.sqrt(2.0 * math.pi))))
        extra = jnp.where(iota((16, preact.shape[1]), 0) < 3, 1.0, 0.0).astype(BF16)
        hiddens.append(jnp.concatenate([(preact * cdf).astype(BF16), extra], 0))
        kernels.append(dot(wo_ref[...], hiddens[-1]))
    cots = [here[:ch] for here in heres]
    grads = [(kernel * cot).astype(BF16) for kernel, cot in zip(kernels, cots)]
    return rels, cots, features, slopes, hiddens, grads


def entries_backward(windows, rels, cots, features, slopes, hiddens, wt_ref, totals_ref):
    ch = cots[0].shape[0]
    hid = slopes[0].shape[0]
    feats = [dot(window, one_hot(rel, SPAN)) for window, rel in zip(windows, rels)]
    grad_kernels = [(feat * cot).astype(BF16) for feat, cot in zip(feats, cots)]
    grad_pres = [dot(wt_ref[...], g) * slope for g, slope in zip(grad_kernels, slopes)]
    totals_ref[0:ch, 0 : hid + 16] += sum(dot(g, hidden, NT) for g, hidden in zip(grad_kernels, hiddens))
    small = None
    for feature, grad_pre in zip(features, grad_pres):
        hi = grad_pre.astype(BF16)
        low = (grad_pre - hi.astype(F32)).astype(BF16)
        term = dot(feature, hi, NT) + dot(feature, low, NT)
        small = term if small is None else small + term
    totals_ref[ch : ch + 16, 0:hid] += small


MESH_ID = pl.DeviceIdType.MESH


class Place:
    def __init__(self):
        self.x, self.y, self.h, self.c = (lax.axis_index(name) for name in PB)
        self.g = lax.axis_index("ga")
        self.first = self.x * (1 - self.c) + self.y * self.c
        self.second = self.y * (1 - self.c) + self.x * self.c

    def at(self, first=None, second=None, h=None, c=None, g=None):
        first = self.first if first is None else first
        second = self.second if second is None else second
        core = self.c
        return (
            first * (1 - core) + second * core,
            second * (1 - core) + first * core,
            self.h if h is None else h,
            core if c is None else c,
            self.g if g is None else g,
        )

    def sibling(self):
        return (self.x, self.y, self.h, 1 - self.c, self.g)


def greet(devices):
    barrier = pltpu.get_barrier_semaphore()
    for device in devices:
        pl.semaphore_signal(barrier, inc=1, device_id=device, device_id_type=MESH_ID)
    return lambda: pl.semaphore_wait(barrier, len(devices))


def load_all(pairs, sems):
    copies = [
        pltpu.make_async_copy(source, target, sems.at[n]) for n, (source, target) in enumerate(pairs)
    ]
    for copy in copies:
        copy.start()
    return copies


def gather_kernel(
    *refs,
):
    sources = refs[:10]
    targets = refs[22:32]
    offsets_ref, points_ref, cot_ref, slab_ref, rel_ref, w_in_ref, b_in_ref, w_out_ref, b_out_ref, block_ref = targets
    (
    out_ref, spread_ref, info_ref, count_ref, near_ref, cots_ref, feature_ref, slope_ref, hidden_ref,
    a_ref, wo_ref, wt_ref,
    ) = refs[10:22]
    load_sem, send_sem, recv_sem = refs[32:]
    me = Place()
    loads = load_all(list(zip(sources, targets)), load_sem)
    wide = block_ref.shape[1]
    cells = out_ref.shape[1]
    tiles = slab_ref.shape[1] // TILE
    sends = []

    def number(first, second, h, c):
        x = first * (1 - me.c) + second * me.c
        y = second * (1 - me.c) + first * me.c
        return ((x * 4 + y) * 2 + h) * 2 + c

    def spot(p):
        return out_ref.at[:, pl.ds(pl.multiple_of(p * wide, wide), wide)]

    def send(source, p, device):
        copy = pltpu.make_async_remote_copy(
            src_ref=source,
            dst_ref=spot(p),
            send_sem=send_sem.at[len(sends)],
            recv_sem=recv_sem.at[p],
            device_id=device,
            device_id_type=MESH_ID,
        )
        copy.start()
        sends.append(copy)

    def arrived(p):
        pltpu.make_async_remote_copy(
            src_ref=spot(p),
            dst_ref=spot(p),
            send_sem=send_sem.at[0],
            recv_sem=recv_sem.at[p],
            device_id=me.sibling(),
            device_id_type=MESH_ID,
        ).wait_recv()

    def forward(first_group, last_group):
        def group_step(g, carry):
            ids = [g * GROUP + n for n in range(GROUP)]
            columns = []
            for t in ids:
                lanes = pl.ds(pl.multiple_of(t * TILE, TILE), TILE)
                columns.append(query_columns(points_ref[:, lanes], cot_ref[:, lanes]))
            infos = [jnp.concatenate([info_ref[t, 0:1, :], info_ref[t, 1:2, :]], 1) for t in ids]
            results = entries_forward(
                infos, [offsets_ref[0, t] for t in ids], cells, me.g, columns, a_ref, wo_ref
            )
            for t, rel, cot, feature, slope, hidden, grad in zip(ids, *results):
                spread_ref[t] = dot(grad, one_hot(rel, SPAN), NT)
                near_ref[t] = rel
                cots_ref[t] = cot.astype(BF16)
                feature_ref[t] = feature
                slope_ref[t] = slope
                hidden_ref[t] = hidden
            return carry

        lax.fori_loop(first_group, last_group, group_step, 0)

    steps = (1, 3, 2)
    near = [me.at(first=(me.first + n) % 4) for n in steps]
    far = [me.at(second=(me.second + n) % 4) for n in steps]
    across = me.at(h=1 - me.h)
    all_here = greet([me.sibling(), across] + near + far)
    mine = number(me.first, me.second, me.h, me.c)
    groups = tiles // GROUP
    for copy in loads:
        copy.wait()
    weight_prologue(w_in_ref, b_in_ref, w_out_ref, b_out_ref, a_ref, wo_ref, wt_ref)
    compact(me.g, slab_ref, rel_ref, info_ref, count_ref)
    all_here()
    for device in [across] + near + far + [me.sibling()]:
        send(block_ref, mine, device)
    out_ref[:, pl.ds(pl.multiple_of(mine * wide, wide), wide)] = block_ref[...]

    def pass_on(p, devices):
        arrived(p)
        for device in devices + [me.sibling()]:
            send(spot(p), p, device)

    other = 1 - me.h
    forward(0, groups // 2)
    for n in steps:
        pass_on(number((me.first + n) % 4, me.second, me.h, me.c), far)
    forward(groups // 2, groups)
    pass_on(number(me.first, me.second, other, me.c), near + far)
    for n in steps:
        for m in (0, 1, 3, 2):
            pass_on(number((me.first + m) % 4, (me.second + n) % 4, me.h, me.c), [])
    for n in steps:
        pass_on(number((me.first + n) % 4, me.second, other, me.c), far)
    for n in steps:
        for m in (0, 1, 3, 2):
            pass_on(number((me.first + m) % 4, (me.second + n) % 4, other, me.c), [])
    for x in range(4):
        for y in range(4):
            for h in range(2):
                arrived(((x * 4 + y) * 2 + h) * 2 + 1 - me.c)
    for copy in sends:
        copy.wait_send()


def gather_and_forward(offsets, points, cot, slabs, rels, w_in, b_in, w_out, b_out, block, owners):
    ch, wide = block.shape
    hid = w_in.shape[1]
    tiles = slabs.shape[1] // TILE
    vmem = pl.BlockSpec(memory_space=pltpu.VMEM)
    shape = jax.ShapeDtypeStruct
    return pl.pallas_call(
        gather_kernel,
        out_shape=(
            shape((ch, wide * owners), BF16),
            shape((tiles, ch, SPAN), F32),
            shape((tiles, KN, TILE), F32),
            shape((8, TILE), I32),
            shape((tiles, 1, BLOCK), F32),
            shape((tiles, ch, BLOCK), BF16),
            shape((tiles, 16, BLOCK), BF16),
            shape((tiles, hid, BLOCK), F32),
            shape((tiles, hid + 16, BLOCK), BF16),
            shape((hid, 48), BF16),
            shape((ch, hid + 16), BF16),
            shape((hid, ch), BF16),
        ),
        in_specs=[pl.BlockSpec(memory_space=pltpu.HBM)] * 10,
        out_specs=(vmem,) * 12,
        scratch_shapes=[pltpu.SMEM(offsets.shape, I32)]
        + [
            pltpu.VMEM(value.shape, value.dtype)
            for value in (points, cot, slabs, rels, w_in, b_in, w_out, b_out, block)
        ]
        + [pltpu.SemaphoreType.DMA((n,)) for n in (10, 63, 64)],
        compiler_params=pltpu.CompilerParams(
            collective_id=0, has_side_effects=True, vmem_limit_bytes=40 << 20
        ),
        name="gather_and_forward",
    )(offsets, points, cot, slabs, rels, w_in, b_in, w_out, b_out, block)


def local_kernel(
    counts_ref, offsets_hbm, points_ref, cot_ref, feats_ref, spread_ref, info_ref, a_ref, wo_ref, wt_ref,
    partial_ref, totals_ref, window_ref,
    acc_ref, offsets_ref, some_points_ref, some_cot_ref, sem,
):
    slab_here = lax.axis_index("ga")
    cells = acc_ref.shape[1]
    tiles = spread_ref.shape[0]
    (load,) = load_all([(offsets_hbm, offsets_ref)], sem)
    acc_ref[...] = jnp.zeros_like(acc_ref)
    totals_ref[...] = jnp.zeros_like(totals_ref)
    load.wait()

    def tile_step(t, carry):
        start = offsets_ref[0, t]
        window = pl.ds(pl.multiple_of(first_cell(start, cells), TILE), SPAN)
        acc_ref[:, window] += spread_ref[t]
        window_ref[t] = feats_ref[:, window]

        def block_step(n, carry):
            lanes = pl.ds(pl.multiple_of(t * TILE, TILE), TILE)
            for copy in load_all(
                [(points_ref.at[:, lanes], some_points_ref), (cot_ref.at[:, lanes], some_cot_ref)], sem
            ):
                copy.wait()
            columns = query_columns(some_points_ref[...], some_cot_ref[...])
            info = jnp.concatenate(
                [info_ref[t, pl.ds(2 * n, 1), :], info_ref[t, pl.ds(2 * n + 1, 1), :]], 1
            )
            rels, cots, features, slopes, hiddens, grads = entries_forward(
                [info], [start], cells, slab_here, [columns], a_ref, wo_ref
            )
            acc_ref[:, window] += dot(grads[0], one_hot(rels[0], SPAN), NT)
            entries_backward(
                [feats_ref[:, window]], rels, cots, features, slopes, hiddens, wt_ref, totals_ref
            )
            return carry

        return lax.fori_loop(1, (counts_ref[0, t] + (BLOCK - 1)) // BLOCK, block_step, carry)

    lax.fori_loop(0, tiles, tile_step, 0)
    wide = partial_ref.shape[-1]
    for p, (x, y, h, c) in enumerate(itertools.product(range(4), range(4), range(2), range(2))):
        first, second = ((x, y), (y, x))[c]
        partial_ref[c, first, second, h] = acc_ref[:, p * wide : (p + 1) * wide].astype(BF16)


def local_sums(offsets, counts, points, cot, feats, spread, info, a, wo, wt):
    ch, cells = feats.shape
    vmem = pl.BlockSpec(memory_space=pltpu.VMEM)
    return pl.pallas_call(
        local_kernel,
        out_shape=(
            jax.ShapeDtypeStruct((2, 4, 4, 2, ch, cells // 64), BF16),
            jax.ShapeDtypeStruct((ch + 16, TILE), F32),
            jax.ShapeDtypeStruct((spread.shape[0], ch, SPAN), BF16),
        ),
        in_specs=[pl.BlockSpec(memory_space=pltpu.SMEM)] + [pl.BlockSpec(memory_space=pltpu.HBM)] * 3 + [vmem] * 6,
        out_specs=(vmem, vmem, vmem),
        scratch_shapes=[
            pltpu.VMEM((ch, cells), F32),
            pltpu.SMEM(offsets.shape, I32),
            pltpu.VMEM((points.shape[0], TILE), F32),
            pltpu.VMEM((ch, TILE), BF16),
            pltpu.SemaphoreType.DMA((2,)),
        ],
        compiler_params=pltpu.CompilerParams(vmem_limit_bytes=40 << 20),
        name="local_sums",
    )(counts, offsets, points, cot, feats, spread, info, a, wo, wt)


def reduce_kernel(
    partial_ref, beyond_ref, window_ref, near_ref, cots_ref, feature_ref, slope_ref, hidden_ref, wt_ref,
    out_ref, sums_ref,
    totals_ref,
    r0_ref, s0_ref, r1_ref, s1_ref, r2_ref, s2_ref, r3_ref,
    ta_ref, tf_ref, ts_ref, tz_ref, th_ref,
    sem0, sem1, sem2, sem3, tsem_a, tsem_f, tsem_s, tsem_z, tsem_h,
):
    me = Place()
    half = ta_ref.shape[0]
    sends = []

    def send(source, target, sems, device, recv_index, send_index):
        copy = pltpu.make_async_remote_copy(
            src_ref=source,
            dst_ref=target,
            send_sem=sems.at[(0,) + send_index],
            recv_sem=sems.at[(1,) + recv_index],
            device_id=device,
            device_id_type=MESH_ID,
        )
        copy.start()
        sends.append(copy)

    def arrived(target, sems, recv_index):
        pltpu.make_async_remote_copy(
            src_ref=target,
            dst_ref=target,
            send_sem=sems.at[(0,) + recv_index],
            recv_sem=sems.at[(1,) + recv_index],
            device_id=me.sibling(),
            device_id_type=MESH_ID,
        ).wait_recv()

    steps = (2, 1, 3)
    firsts = [(me.first + n) % 4 for n in steps]
    seconds = [(me.second + n) % 4 for n in steps]
    depth = me.h * 4 + me.g
    depths = [(depth + n) % 8 for n in range(1, 8)]
    line = [me.at(h=d // 4, g=d % 4) for d in depths]
    across = me.at(h=1 - me.h)
    all_here = greet(
        [me.sibling()]
        + [me.at(first=f) for f in firsts]
        + [me.at(second=s) for s in seconds]
        + line
    )

    tiles = near_ref.shape[0]

    def backward(first_group, last_group):
        def group_step(g, carry):
            ids = [g * GROUP + n for n in range(GROUP)]
            entries_backward(
                [window_ref[t] for t in ids],
                [near_ref[t] for t in ids],
                [cots_ref[t].astype(F32) for t in ids],
                [feature_ref[t] for t in ids],
                [slope_ref[t] for t in ids],
                [hidden_ref[t] for t in ids],
                wt_ref,
                totals_ref,
            )
            return carry

        lax.fori_loop(first_group, last_group, group_step, 0)

    own_half = pl.ds(pl.multiple_of(me.c * half, 8), half)
    other_half = pl.ds(pl.multiple_of((1 - me.c) * half, 8), half)
    totals_ref[...] = beyond_ref[...]
    backward(0, tiles // GROUP)
    all_here()
    send(totals_ref.at[other_half], ta_ref, tsem_a, me.sibling(), (0,), (0,))
    for m in steps + (0,):
        for n in steps + (0,):
            f, s = (me.second + n) % 4, (me.first + m) % 4
            send(partial_ref.at[1 - me.c, f, s], r0_ref.at[f, s], sem0, me.sibling(), (f, s), (f, s))
    for m in steps + (0,):
        s = (me.second + m) % 4
        for n, f in zip(steps, firsts):
            arrived(r0_ref.at[f, s], sem0, (f, s))
            s0_ref[n - 1, s] = (partial_ref[me.c, f, s].astype(F32) + r0_ref[f, s].astype(F32)).astype(BF16)
            send(s0_ref.at[n - 1, s], r1_ref.at[3 - n, s], sem1, me.at(first=f), (3 - n, s), (n - 1, s))
    arrived(ta_ref, tsem_a, (0,))
    tf_ref[me.first] = totals_ref[own_half] + ta_ref[...]
    for n, f in zip(steps, firsts):
        send(tf_ref.at[me.first], tf_ref.at[me.first], tsem_f, me.at(first=f), (me.first,), (n,))

    def collect(s):
        arrived(r0_ref.at[me.first, s], sem0, (me.first, s))
        total = partial_ref[me.c, me.first, s].astype(F32) + r0_ref[me.first, s].astype(F32)
        for n in range(3):
            arrived(r1_ref.at[n, s], sem1, (n, s))
            total += r1_ref[n, s].astype(F32)
        return total

    for n, s in zip(steps, seconds):
        s1_ref[n - 1] = collect(s).astype(BF16)
        send(s1_ref.at[n - 1], r2_ref.at[3 - n], sem2, me.at(second=s), (3 - n,), (n - 1,))
        if n == steps[0]:
            for f in firsts:
                arrived(tf_ref.at[f], tsem_f, (f,))
            ts_ref[me.second] = tf_ref[0] + tf_ref[1] + tf_ref[2] + tf_ref[3]
            for k, t in zip(steps, seconds):
                send(ts_ref.at[me.second], ts_ref.at[me.second], tsem_s, me.at(second=t), (me.second,), (k,))
    total = collect(me.second)
    for s in seconds:
        arrived(ts_ref.at[s], tsem_s, (s,))
    tz_ref[depth] = ts_ref[0] + ts_ref[1] + ts_ref[2] + ts_ref[3]
    for n, device in enumerate(line):
        send(tz_ref.at[depth], tz_ref.at[depth], tsem_z, device, (depth,), (n,))
    for n in range(3):
        arrived(r2_ref.at[n], sem2, (n,))
        total += r2_ref[n].astype(F32)
    s2_ref[...] = total
    s1_ref[3, 0] = s2_ref[1 - me.h].astype(BF16)
    send(s1_ref.at[3, 0], r3_ref, sem3, across, (0,), (0,))
    for d in depths:
        arrived(tz_ref.at[d], tsem_z, (d,))
    total = tz_ref[0]
    for d in range(1, 8):
        total += tz_ref[d]
    th_ref[me.c] = total
    send(th_ref.at[me.c], th_ref.at[me.c], tsem_h, me.sibling(), (me.c,), (0,))
    arrived(r3_ref, sem3, (0,))
    out_ref[...] = s2_ref[me.h] + r3_ref[...].astype(F32)
    arrived(th_ref.at[1 - me.c], tsem_h, (1 - me.c,))
    sums_ref[0:half] = th_ref[0]
    sums_ref[half : 2 * half] = th_ref[1]
    for copy in sends:
        copy.wait_send()


def reduce_and_backward(partial, totals, windows, near, cots, feature, slope, hidden, wt):
    ch, wide = partial.shape[-2:]
    rows, lanes = totals.shape
    half = rows // 2
    vmem = pl.BlockSpec(memory_space=pltpu.VMEM)
    dma = pltpu.SemaphoreType.DMA
    return pl.pallas_call(
        reduce_kernel,
        out_shape=(
            jax.ShapeDtypeStruct((ch, wide), F32),
            jax.ShapeDtypeStruct((rows, lanes), F32),
        ),
        in_specs=[vmem] * 9,
        out_specs=(vmem, vmem),
        scratch_shapes=[
            pltpu.VMEM((rows, lanes), F32),
            pltpu.VMEM((4, 4, 2, ch, wide), BF16),
            pltpu.VMEM((3, 4, 2, ch, wide), BF16),
            pltpu.VMEM((3, 4, 2, ch, wide), BF16),
            pltpu.VMEM((4, 2, ch, wide), BF16),
            pltpu.VMEM((3, 2, ch, wide), BF16),
            pltpu.VMEM((2, ch, wide), F32),
            pltpu.VMEM((ch, wide), BF16),
            pltpu.VMEM((half, lanes), F32),
            pltpu.VMEM((4, half, lanes), F32),
            pltpu.VMEM((4, half, lanes), F32),
            pltpu.VMEM((8, half, lanes), F32),
            pltpu.VMEM((2, half, lanes), F32),
            dma((2, 4, 4)),
            dma((2, 3, 4)),
            dma((2, 3)),
            dma((2, 1)),
            dma((2, 1)),
            dma((2, 4)),
            dma((2, 4)),
            dma((2, 8)),
            dma((2, 2)),
        ],
        compiler_params=pltpu.CompilerParams(
            collective_id=1, has_side_effects=True, vmem_limit_bytes=40 << 20
        ),
        name="reduce_and_backward",
    )(partial, totals, windows, near, cots, feature, slope, hidden, wt)


def final_kernel(scale, owned_ref, sums_ref, grid_ref, w_in_ref, b_in_ref, w_out_ref, b_out_ref, sem):
    copy = pltpu.make_async_copy(owned_ref, grid_ref, sem)
    copy.start()
    ch, hid = w_out_ref.shape
    outer = sums_ref[0:ch] * scale
    rows = sums_ref[ch : ch + 16, 0:hid] * scale
    w_out_ref[...] = outer[:, 0:hid]
    turned = jnp.concatenate([outer, jnp.zeros((TILE - ch, TILE), F32)], 0).T
    b_out_ref[...] = turned[hid : hid + 1, 0:ch]
    w_in_ref[...] = jnp.concatenate([rows[0:3] + rows[3:6] + rows[6:9], rows[9:12]], 0)
    b_in_ref[...] = rows[12:13]
    copy.wait()


def final_form(owned, sums, scale, hid):
    ch = owned.shape[0]
    vmem = pl.BlockSpec(memory_space=pltpu.VMEM)
    shape = jax.ShapeDtypeStruct
    return pl.pallas_call(
        functools.partial(final_kernel, scale),
        out_shape=(
            shape(owned.shape, F32),
            shape((6, hid), F32),
            shape((1, hid), F32),
            shape((ch, hid), F32),
            shape((1, ch), F32),
        ),
        in_specs=[vmem, vmem],
        out_specs=(pl.BlockSpec(memory_space=pltpu.HBM),) + (vmem,) * 4,
        scratch_shapes=[pltpu.SemaphoreType.DMA],
        name="final_form",
    )(owned, sums)


def shards(query_points, cotangent, slab_ids, rel_cells, offsets, latent, w_in, b_in, w_out, b_out):
    feats, spread, info, counts, near, cots, feature, slope, hidden, a, wo, wt = gather_and_forward(
        offsets, query_points, cotangent, slab_ids, rel_cells,
        w_in.T, b_in[None], w_out, b_out[None], latent[0], lax.axis_size(PB),
    )
    partial, totals, windows = local_sums(
        offsets, counts, query_points, cotangent, feats, spread, info, a, wo, wt
    )
    owned, totals = reduce_and_backward(
        partial, totals, windows, near, cots, feature, slope, hidden, wt
    )
    scale = float(query_points.shape[1] * lax.axis_size(PB)) ** (-0.5)
    grid, w_in_grad, b_in_grad, w_out_grad, b_out_grad = final_form(owned, totals, scale, w_out.shape[1])
    return grid[None], w_in_grad.T, b_in_grad[0], w_out_grad, b_out_grad[0]


def solution(mesh):
    finer = Mesh(
        mesh.devices.reshape(4, 4, 2, 2, mesh.shape["ga"]), ("pb_0", "pb_1", "pb_2", "pb_3", "ga")
    )
    in_specs = (
        P(None, PB),
        P(None, PB),
        P(None, PB),
        P(None, PB),
        P("ga", PB),
        P("ga", None, PB),
        P(),
        P(),
        P(),
        P(),
    )
    out_specs = (P("ga", None, PB), P(), P(), P(), P())
    return jax.shard_map(
        shards, mesh=finer, in_specs=in_specs, out_specs=out_specs, check_vma=False
    )
```
